16 devices in a mesh: dp: 2 (over z), tp: 8 (over y, x, core).
Axes of the slice: x: 2, y: 2, z: 2, core: 2. Of those that a mesh axis runs over, the one named last changes fastest.
Arguments:
- w_up: bfloat16 [2, 2048, 16384], P(None, None, 'tp')
- w_down: bfloat16 [2, 16384, 2048], P(None, 'tp')
- x_saved: bfloat16 [2, 2, 4096, 2048], P(None, 'dp')
- h_saved: bfloat16 [2, 2, 4096, 16384], P(None, 'dp', None, 'tp')
- grad_out: bfloat16 [2, 4096, 2048], P('dp')
Outputs:
- output 1: bfloat16 [2, 4096, 2048], P('dp')
- output 2: float32 [2, 2048, 16384], P(None, None, 'tp')
- output 3: float32 [2, 16384, 2048], P(None, 'tp')
All inputs are finite; a program needn't handle non-finite values.
Results may differ from the reference program's by a relative error of at most 0.0130822.
Values are sent between devices in bfloat16 or wider.
A program may use at most 1 GiB of HBM per device.

```python
import jax
import jax.numpy as jnp
from jax import lax

LAYER_COUNT = 2
BATCH_ALL = 2
SEQ_LEN = 4096
D = 2048
F = 16384


def gelu_parts(hidden):
    tanh_val = jnp.tanh(0.7978845608028654 * (hidden + 0.044715 * hidden * hidden * hidden))
    gelu_out = 0.5 * hidden * (1.0 + tanh_val)
    gelu_slope = 0.5 * (1.0 + tanh_val) + 0.5 * hidden * (1.0 - tanh_val * tanh_val) * 0.7978845608028654 * (1.0 + 0.134145 * hidden * hidden)
    return gelu_out, gelu_slope


def forward_saved(x_first, w_up, w_down):
    rows_cur = x_first.reshape(BATCH_ALL * SEQ_LEN, D)
    x_list = []
    h_list = []
    for layer_idx in range(LAYER_COUNT):
        hidden = jnp.dot(rows_cur, w_up[layer_idx], preferred_element_type=jnp.float32).astype(jnp.bfloat16)
        gelu_out = gelu_parts(hidden.astype(jnp.float32))[0]
        branch = jnp.dot(gelu_out.astype(jnp.bfloat16), w_down[layer_idx], preferred_element_type=jnp.float32)
        x_list.append(rows_cur)
        h_list.append(hidden)
        rows_cur = (rows_cur.astype(jnp.float32) + branch).astype(jnp.bfloat16)
    x_saved = jnp.stack(x_list).reshape(LAYER_COUNT, BATCH_ALL, SEQ_LEN, D)
    h_saved = jnp.stack(h_list).reshape(LAYER_COUNT, BATCH_ALL, SEQ_LEN, F)
    return x_saved, h_saved


def setup_inputs(seed: int = 0) -> dict:
    root_key = jax.random.key(seed)
    key_x, key_up, key_down, key_grad = jax.random.split(root_key, 4)
    x_first = jax.random.normal(key_x, (BATCH_ALL, SEQ_LEN, D), jnp.float32).astype(jnp.bfloat16)
    w_up = (jax.random.normal(key_up, (LAYER_COUNT, D, F), jnp.float32) * (D ** -0.5)).astype(jnp.bfloat16)
    w_down = (jax.random.normal(key_down, (LAYER_COUNT, F, D), jnp.float32) * (F ** -0.5)).astype(jnp.bfloat16)
    grad_out = jax.random.normal(key_grad, (BATCH_ALL, SEQ_LEN, D), jnp.float32).astype(jnp.bfloat16)
    x_saved, h_saved = forward_saved(x_first, w_up, w_down)
    return {"w_up": w_up, "w_down": w_down, "x_saved": x_saved, "h_saved": h_saved, "grad_out": grad_out}


def reference(w_up, w_down, x_saved, h_saved, grad_out):
    def one_sequence(accums, seq_idx):
        up_acc, down_acc = accums
        grad_cur = grad_out[seq_idx]
        up_new = [None] * LAYER_COUNT
        down_new = [None] * LAYER_COUNT
        for layer_idx in reversed(range(LAYER_COUNT)):
            x_seq = x_saved[layer_idx, seq_idx]
            gelu_out, gelu_slope = gelu_parts(h_saved[layer_idx, seq_idx].astype(jnp.float32))
            act_grad = jnp.dot(grad_cur, w_down[layer_idx].T, preferred_element_type=jnp.float32)
            hid_grad = (act_grad * gelu_slope).astype(jnp.bfloat16)
            part_sum = jnp.dot(hid_grad, w_up[layer_idx].T, preferred_element_type=jnp.float32)
            down_new[layer_idx] = jnp.dot(gelu_out.astype(jnp.bfloat16).T, grad_cur, preferred_element_type=jnp.float32)
            up_new[layer_idx] = jnp.dot(x_seq.T, hid_grad, preferred_element_type=jnp.float32)
            grad_cur = (grad_cur.astype(jnp.float32) + part_sum).astype(jnp.bfloat16)
        return (up_acc + jnp.stack(up_new), down_acc + jnp.stack(down_new)), grad_cur
    zero_acc = (jnp.zeros((LAYER_COUNT, D, F), jnp.float32), jnp.zeros((LAYER_COUNT, F, D), jnp.float32))
    (up_grad, down_grad), grad_in = lax.scan(one_sequence, zero_acc, jnp.arange(BATCH_ALL))
    return grad_in, up_grad, down_grad
```

```python
import jax
import jax.numpy as jnp
from jax import lax
from jax.experimental import pallas as pl
from jax.experimental.pallas import tpu as pltpu
from jax.sharding import PartitionSpec as P

D = 2048
F = 2048
PIECE = 1024
BM = 512
BN = 1024
C0 = 0.7978845608028654
C1 = 0.7978845608028654 * 0.044715
C3 = 0.7978845608028654 * 0.134145
AXES = ("dp", "tp")
VMEM_LIMIT = 60 * 1024 * 1024
BF16 = jnp.bfloat16
NN = (((1,), (0,)), ((), ()))
NT = (((1,), (1,)), ((), ()))
TN = (((0,), (0,)), ((), ()))


def make_perm(fn):
    pairs = []
    for z in range(2):
        for y in range(2):
            for x in range(2):
                for c in range(2):
                    z2, y2, x2, c2 = fn(z, y, x, c)
                    pairs.append((z * 8 + (y * 2 + x) * 2 + c, z2 * 8 + (y2 * 2 + x2) * 2 + c2))
    return pairs


PERM_Z = make_perm(lambda z, y, x, c: (1 - z, y, x, c))
PERM_C = make_perm(lambda z, y, x, c: (z, y, x, 1 - c))
PERM_S1 = make_perm(lambda z, y, x, c: (z, y, 1 - x, c) if c == 0 else (z, 1 - y, x, c))
PERM_S2 = make_perm(lambda z, y, x, c: (z, 1 - y, x, c) if c == 0 else (z, y, 1 - x, c))


def send(value, pairs):
    return lax.ppermute(value, AXES, pairs)


def device_order():
    tp = lax.axis_index("tp")
    z = lax.axis_index("dp")
    y, x, c = tp // 4, (tp // 2) % 2, tp % 2
    first = c == 0
    blocks = [jnp.where(first, x, 2 + y), jnp.where(first, 1 - x, 3 - y), jnp.where(first, 2 + y, x), jnp.where(first, 3 - y, 1 - x)]
    return jnp.stack(blocks + [z, 1 - z]).astype(jnp.int32), jnp.where(first, y, x).astype(jnp.int32)


TOKEN = jax.ShapeDtypeStruct((8, 128), jnp.float32)
TOKEN_SPEC = pl.BlockSpec((8, 128), lambda *g: (0, 0))
ANY_SPEC = pl.BlockSpec(memory_space=pl.ANY)
MINE, THEIRS = 4, 5


def call(body, grid, ins, outs, flops, order, token, aliases=None):
    n_in, n_out = len(ins), len(outs)

    def wrapped(order_ref, *refs):
        token_out = refs[n_in + 1 + n_out]
        token_out[...] = jnp.zeros((8, 128), jnp.float32)
        body(refs[:n_in], refs[n_in + 1:n_in + 1 + n_out])

    return pl.pallas_call(
        wrapped,
        grid_spec=pltpu.PrefetchScalarGridSpec(
            num_scalar_prefetch=1, grid=grid,
            in_specs=[s for _, s in ins] + [ANY_SPEC],
            out_specs=[s for _, s in outs] + [TOKEN_SPEC]),
        out_shape=[s for s, _ in outs] + [TOKEN],
        input_output_aliases={} if aliases is None else {k + 1: v for k, v in aliases.items()},
        compiler_params=pltpu.CompilerParams(vmem_limit_bytes=VMEM_LIMIT),
        cost_estimate=pl.CostEstimate(flops=flops, bytes_accessed=60_000_000, transcendentals=0),
    )(order, *[a for a, _ in ins], token)


class Piece:
    def __init__(self, array, *lead):
        self.array = array
        self.lead = lead

    def spec(self, rows, cols, place):
        n = len(self.lead)

        def index(*args):
            order = args[-1]
            return tuple(order[k[0]] if isinstance(k, tuple) else k for k in self.lead) + place(*args)

        return (self.array, pl.BlockSpec((None,) * n + (rows, cols), index))


def parts(arr):
    return [Piece(arr, k) for k in range(arr.shape[0])]


def whole(*arrs):
    return [Piece(a) for a in arrs]


def natural(arr, *lead):
    return [Piece(arr, *lead, (k,)) for k in range(4)]


def join(refs, axis=0):
    return jnp.concatenate([r[...] for r in refs], axis=axis)


def hidden_grad(order, token, grad, hidden, w_down, layer, half):
    n = len(grad)
    cols = BN if half else F
    groups = n // 2

    def body(ins, outs):
        act = lax.dot_general(join(ins[:n]), ins[2 * n][...], NT, preferred_element_type=jnp.float32)
        h = join(ins[n:2 * n]).astype(jnp.float32)
        h2 = h * h
        t = jnp.tanh(h * (C0 + C1 * h2))
        s = 0.5 + 0.5 * t
        a = h * s
        slope = s + a * ((1.0 - t) * (C0 + C3 * h2))
        outs[0][...] = a.reshape(n, BM // n, BN).astype(BF16)
        d = (act * slope).reshape(n, BM // n, BN).astype(BF16)
        for k in range(groups):
            outs[1 + k][...] = d[2 * k:2 * k + 2]

    ins = [p.spec(BM // n, D, lambda j, i, o: (i, 0)) for p in grad]
    ins += [p.spec(BM // n, BN, lambda j, i, o: (i, j)) for p in hidden]
    ins.append((w_down, pl.BlockSpec((None, BN, D), lambda j, i, o: (layer, o[MINE] if half else j, 0))))

    def out(m):
        return (jax.ShapeDtypeStruct((m, PIECE, cols), BF16), pl.BlockSpec((m, BM // n, BN), lambda j, i, o: (0, i, j)))

    *res, tok = call(body, (cols // BN, n * PIECE // BM), ins, [out(n)] + [out(2)] * groups, 2 * n * PIECE * D * cols, order, token)
    return res[0], res[1:], tok


def hidden_again(order, token, x, w_up, layer, half):
    n = len(x)
    cols = BN if half else F

    def body(ins, outs):
        h = lax.dot_general(join(ins[:n]), ins[n][...], NN, preferred_element_type=jnp.float32)
        outs[0][...] = h.reshape(n, BM // n, BN).astype(BF16)

    ins = [p.spec(BM // n, D, lambda j, i, o: (i, 0)) for p in x]
    ins.append((w_up, pl.BlockSpec((None, D, BN), lambda j, i, o: (layer, 0, o[MINE] if half else j))))
    out = (jax.ShapeDtypeStruct((n, PIECE, cols), BF16), pl.BlockSpec((n, BM // n, BN), lambda j, i, o: (0, i, j)))
    return call(body, (cols // BN, n * PIECE // BM), ins, [out], 2 * n * PIECE * D * cols, order, token)


def back_term(order, token, d_mine, d_core, w_mine, w_core, layer):
    n = 2

    def body(ins, outs):
        left = jnp.concatenate([join(ins[:n]), join(ins[n:2 * n])], axis=1)
        acc = lax.dot_general(left, join(ins[2 * n:2 * n + 2], 1), NT, preferred_element_type=jnp.float32)
        for k in range(n):
            outs[k][...] = acc[k * (BM // n):(k + 1) * (BM // n)].astype(BF16)

    ins = [p.spec(BM // n, F, lambda j, i, o: (i, 0)) for p in parts(d_mine) + parts(d_core)]
    ins += [(w, pl.BlockSpec((None, BN, F), lambda j, i, o: (layer, j, 0))) for w in (w_mine, w_core)]
    outs = [(jax.ShapeDtypeStruct((PIECE, D), BF16), pl.BlockSpec((BM // n, BN), lambda j, i, o: (i, j)))] * n
    return call(body, (D // BN, n * PIECE // BM), ins, outs, 4 * n * PIECE * D * F, order, token)


def weight_grad(order, token, left, right, left_cols, right_cols, bn, ins_more, outs, add, aliases):
    n = len(left)
    (grid_i, at_i), (grid_j, at_j) = left_cols, right_cols

    def body(ins, outs):
        acc = lax.dot_general(join(ins[:n]), join(ins[n:2 * n]), TN, preferred_element_type=jnp.float32)
        if add:
            acc = acc + ins[2 * n][...]
        for o in outs:
            o[...] = acc

    ins = [p.spec(PIECE, BN, lambda i, j, o: (0, at_i(i, o))) for p in left]
    ins += [p.spec(PIECE, bn, lambda i, j, o: (0, at_j(j, o))) for p in right]
    return call(body, (grid_i, grid_j), ins + ins_more, outs, 2 * n * PIECE * grid_i * BN * grid_j * bn, order, token,
                None if aliases is None else {2 * n + k: v for k, v in aliases.items()})


STACK = jax.ShapeDtypeStruct((2, 2048, 2048), jnp.float32)


def weight_full(order, token, left, right, total, add):
    tile = pl.BlockSpec((None, BN, BN), lambda i, j, o: (0, i, j))
    step = (2, lambda k, o: k)
    return weight_grad(order, token, left, right, step, step, BN, [(total, tile if add else ANY_SPEC)], [(STACK, tile)], add, {0: 0})


def weight_half(order, token, left, right, down, prev):
    bn = 512
    if down:
        shape = jax.ShapeDtypeStruct((BN, D), jnp.float32)
        cols = ((1, lambda k, o: o[MINE] if prev is None else 0), (4, lambda k, o: k))
        at = lambda i, j, o: (1, o[MINE], j)
    else:
        shape = jax.ShapeDtypeStruct((D, BN), jnp.float32)
        cols = ((2, lambda k, o: k), (2, lambda k, o: 2 * o[MINE] + k if prev is None else k))
        at = lambda i, j, o: (1, i, 2 * o[MINE] + j)
    tile = pl.BlockSpec((BN, bn), lambda i, j, o: (i, j))
    outs = [(shape, tile)]
    if prev is not None:
        outs.append((STACK, pl.BlockSpec((None, BN, bn), at)))
    return weight_grad(order, token, left, right, *cols, bn, [] if prev is None else [(prev, tile)], outs, prev is not None, None)


def finish(order, token, pieces, down_in, up_in, down, up):
    def body(ins, outs):
        i = pl.program_id(0)
        for k in range(4):
            @pl.when(i // 2 == k)
            def _(k=k):
                outs[0][...] = ins[k][...]
        outs[1][...] = ins[4][...]
        outs[2][...] = ins[5][...]

    ins = [p.spec(BM, D, lambda i, o, k=k: (jnp.clip(i - 2 * k, 0, 1), 0)) for k, p in enumerate(pieces)]
    ins += [(down_in, pl.BlockSpec((128, D), lambda i, o: (i, 0))), (up_in, pl.BlockSpec((256, BN), lambda i, o: (i, 0)))]
    ins += [(down, ANY_SPEC), (up, ANY_SPEC)]
    outs = [(jax.ShapeDtypeStruct((4, PIECE, D), BF16), pl.BlockSpec((None, BM, D), lambda i, o: (o[i // 2], i % 2, 0))),
            (STACK, pl.BlockSpec((None, 128, D), lambda i, o: (1, 8 * o[THEIRS] + i, 0))),
            (STACK, pl.BlockSpec((None, 256, BN), lambda i, o: (1, i, o[THEIRS])))]
    return call(body, (8,), ins, outs, 1000, order, token, {6: 1, 7: 2})


def f32(v):
    return v.astype(jnp.float32)


def solution(mesh):
    def steps(w_up, w_down, x_saved, h_saved, grad_out):
        order, sub = device_order()
        tok = jnp.zeros((8, 128), jnp.float32)
        x_nat = x_saved.reshape(2, 4, PIECE, D)
        h_nat = h_saved.reshape(2, 4, PIECE, F)
        g_nat = grad_out.reshape(4, PIECE, D)

        def my_half(block, which):
            return lax.dynamic_slice(block, (which * BM, 0), (BM, D))

        def both_halves(mine, other):
            return jnp.where(sub == 0, jnp.concatenate([mine, other]), jnp.concatenate([other, mine]))

        def own_block(arr, *lead):
            idx = tuple(lead) + (order[0], 0, 0)
            return lax.dynamic_slice(arr, idx, (1,) * (len(lead) + 1) + (PIECE, D)).reshape(PIECE, D)

        def summed(p02, near, which):
            return f32(my_half(p02, which)) + f32(my_half(near, which))

        x1z = send(own_block(x_nat, 1), PERM_Z)
        w_core = send(w_up, PERM_C)
        g2mine = own_block(g_nat)
        g2z = send(g2mine, PERM_Z)
        g2 = natural(g_nat)
        a1, (dm, do), tok = hidden_grad(order, tok, g2, natural(h_nat, 1), w_down, 1, False)
        dc = send(do, PERM_C)
        down_h, tok = weight_half(order, tok, parts(a1), g2, True, None)
        x1c0 = send(x1z, PERM_C)
        x1s = send(x1z, PERM_S1)
        p02, p13, tok = back_term(order, tok, dm, dc, w_up, w_core, 1)
        near = send(p13, PERM_S1)
        up_h, tok = weight_half(order, tok, natural(x_nat, 1), parts(dm) + parts(do), False, None)
        x1c1 = send(x1s, PERM_C)
        x0z = send(own_block(x_nat, 0), PERM_Z)
        hp, tok = hidden_again(order, tok, whole(x1z, x1c0, x1s, x1c1), w_up, 1, True)
        g2c0 = send(g2z, PERM_C)
        g2s = send(g2z, PERM_S1)
        far = send(summed(p02, near, 1 - sub).astype(BF16), PERM_S2)
        apa, (dpa,), tok = hidden_grad(order, tok, whole(g2z, g2c0), [Piece(hp, 0), Piece(hp, 1)], w_down, 1, True)
        g2c1 = send(g2s, PERM_C)
        g1m0 = (f32(my_half(g2mine, sub)) + (summed(p02, near, sub) + f32(far))).astype(BF16)
        g1m2 = send(g1m0, PERM_S2)
        apb, (dpb,), tok = hidden_grad(order, tok, whole(g2s, g2c1), [Piece(hp, 2), Piece(hp, 3)], w_down, 1, True)
        g1mine = both_halves(g1m0, g1m2)
        g1s = send(g1mine, PERM_S1)
        g1c0 = send(g1mine, PERM_C)
        g1zp = send(g1mine, PERM_Z)
        down_h, down, tok = weight_half(order, tok, parts(apa) + parts(apb), whole(g2z, g2c0, g2s, g2c1), True, down_h)
        down_in = send(down_h, PERM_Z)
        up_h, up, tok = weight_half(order, tok, whole(x1z, x1c0, x1s, x1c1), parts(dpa) + parts(dpb), False, up_h)
        g1c1 = send(g1s, PERM_C)
        up_in = send(up_h, PERM_Z)

        g1 = whole(g1mine, g1s, g1c0, g1c1)
        a0, (dm, do), tok = hidden_grad(order, tok, g1, natural(h_nat, 0), w_down, 0, False)
        dc = send(do, PERM_C)
        x0c0 = send(x0z, PERM_C)
        x0s = send(x0z, PERM_S1)
        down, tok = weight_full(order, tok, parts(a0), g1, down, False)
        x0c1 = send(x0s, PERM_C)
        g1cp0 = send(g1zp, PERM_C)
        g1sp = send(g1zp, PERM_S1)
        p02, p13, tok = back_term(order, tok, dm, dc, w_up, w_core, 0)
        near = send(p13, PERM_S1)
        g1cp1 = send(g1sp, PERM_C)
        up, tok = weight_full(order, tok, natural(x_nat, 0), parts(dm) + parts(do), up, False)
        far = send(summed(p02, near, 1 - sub).astype(BF16), PERM_S2)
        hp, tok = hidden_again(order, tok, whole(x0z, x0c0, x0s, x0c1), w_up, 0, False)
        g0m0 = (f32(g1m0) + (summed(p02, near, sub) + f32(far))).astype(BF16)
        g0m2 = send(g0m0, PERM_S2)
        g1p = whole(g1zp, g1cp0, g1sp, g1cp1)
        ap, (dma, dmb), tok = hidden_grad(order, tok, g1p, parts(hp), w_down, 0, False)
        g0mine = both_halves(g0m0, g0m2)
        g0s = send(g0mine, PERM_S1)
        g0c0 = send(g0mine, PERM_C)
        down, tok = weight_full(order, tok, parts(ap), g1p, down, True)
        g0c1 = send(g0s, PERM_C)
        up, tok = weight_full(order, tok, whole(x0z, x0c0, x0s, x0c1), parts(dma) + parts(dmb), up, True)
        grad_in, down, up, tok = finish(order, tok, whole(g0mine, g0s, g0c0, g0c1), down_in, up_in, down, up)
        return grad_in.reshape(1, 4 * PIECE, D), up, down

    body = jax.shard_map(
        steps, mesh=mesh,
        in_specs=(P(None, None, "tp"), P(None, "tp", None), P(None, "dp", None, None), P(None, "dp", None, "tp"), P("dp", None, None)),
        out_specs=(P("dp", None, None), P(None, None, "tp"), P(None, "tp", None)), check_vma=False)
    shapes = ((2, D, 16384), (2, 16384, D), (2, 2, 4096, D), (2, 2, 4096, 16384), (2, 4096, D))
    jax.eval_shape(body, *[jax.ShapeDtypeStruct(s, BF16) for s in shapes])
    return body
```

```python
import jax
import jax.numpy as jnp
from jax import lax
from jax.experimental import pallas as pl
from jax.experimental.pallas import tpu as pltpu
from jax.sharding import PartitionSpec as P

D = 2048
F = 2048
PIECE = 1024
BM = 512
BN = 1024
C0 = 0.7978845608028654
C1 = 0.7978845608028654 * 0.044715
C3 = 0.7978845608028654 * 0.134145
AXES = ("dp", "tp")
VMEM_LIMIT = 60 * 1024 * 1024
BF16 = jnp.bfloat16
NN = (((1,), (0,)), ((), ()))
NT = (((1,), (1,)), ((), ()))
TN = (((0,), (0,)), ((), ()))


def make_perm(fn):
    pairs = []
    for z in range(2):
        for y in range(2):
            for x in range(2):
                for c in range(2):
                    z2, y2, x2, c2 = fn(z, y, x, c)
                    pairs.append((z * 8 + (y * 2 + x) * 2 + c, z2 * 8 + (y2 * 2 + x2) * 2 + c2))
    return pairs


PERM_Z = make_perm(lambda z, y, x, c: (1 - z, y, x, c))
PERM_C = make_perm(lambda z, y, x, c: (z, y, x, 1 - c))
PERM_S1 = make_perm(lambda z, y, x, c: (z, y, 1 - x, c) if c == 0 else (z, 1 - y, x, c))
PERM_S2 = make_perm(lambda z, y, x, c: (z, 1 - y, x, c) if c == 0 else (z, y, 1 - x, c))


def send(value, pairs):
    return lax.ppermute(value, AXES, pairs)


def device_order():
    tp = lax.axis_index("tp")
    z = lax.axis_index("dp")
    y, x, c = tp // 4, (tp // 2) % 2, tp % 2
    first = c == 0
    blocks = [jnp.where(first, x, 2 + y), jnp.where(first, 1 - x, 3 - y), jnp.where(first, 2 + y, x), jnp.where(first, 3 - y, 1 - x)]
    return jnp.stack(blocks + [z, 1 - z]).astype(jnp.int32), jnp.where(first, y, x).astype(jnp.int32)


TOKEN = jax.ShapeDtypeStruct((8, 128), jnp.float32)
TOKEN_SPEC = pl.BlockSpec((8, 128), lambda *g: (0, 0))
ANY_SPEC = pl.BlockSpec(memory_space=pl.ANY)
MINE, THEIRS = 4, 5


def call(body, grid, ins, outs, flops, order, token, aliases=None):
    n_in, n_out = len(ins), len(outs)

    def wrapped(order_ref, *refs):
        token_out = refs[n_in + 1 + n_out]
        token_out[...] = jnp.zeros((8, 128), jnp.float32)
        body(refs[:n_in], refs[n_in + 1:n_in + 1 + n_out])

    return pl.pallas_call(
        wrapped,
        grid_spec=pltpu.PrefetchScalarGridSpec(
            num_scalar_prefetch=1, grid=grid,
            in_specs=[s for _, s in ins] + [ANY_SPEC],
            out_specs=[s for _, s in outs] + [TOKEN_SPEC]),
        out_shape=[s for s, _ in outs] + [TOKEN],
        input_output_aliases={} if aliases is None else {k + 1: v for k, v in aliases.items()},
        compiler_params=pltpu.CompilerParams(vmem_limit_bytes=VMEM_LIMIT),
        cost_estimate=pl.CostEstimate(flops=flops, bytes_accessed=60_000_000, transcendentals=0),
    )(order, *[a for a, _ in ins], token)


class Piece:
    def __init__(self, array, *lead):
        self.array = array
        self.lead = lead

    def spec(self, rows, cols, place):
        n = len(self.lead)

        def index(*args):
            order = args[-1]
            return tuple(order[k[0]] if isinstance(k, tuple) else k for k in self.lead) + place(*args)

        return (self.array, pl.BlockSpec((None,) * n + (rows, cols), index))


def parts(arr):
    return [Piece(arr, k) for k in range(arr.shape[0])]


def whole(*arrs):
    return [Piece(a) for a in arrs]


def natural(arr, *lead):
    return [Piece(arr, *lead, (k,)) for k in range(4)]


def join(refs, axis=0):
    return jnp.concatenate([r[...] for r in refs], axis=axis)


def hidden_grad(order, token, grad, hidden, w_down, layer, half, keep=False, put=None):
    n = len(grad)
    cols = BN if half else F
    groups = n // 2

    def body(ins, outs):
        act = lax.dot_general(join(ins[:n]), ins[2 * n][...], NT, preferred_element_type=jnp.float32)
        h = join(ins[n:2 * n]).astype(jnp.float32)
        h2 = h * h
        t = jnp.tanh(h * (C0 + C1 * h2))
        s = 0.5 + 0.5 * t
        a = h * s
        slope = s + a * ((1.0 - t) * (C0 + C3 * h2))
        outs[0][...] = a.reshape(n, BM // n, BN).astype(BF16)
        d = (act * slope).reshape(n, BM // n, BN).astype(BF16)
        for k in range(groups):
            outs[1 + k][...] = d[2 * k:2 * k + 2]
        if keep:
            outs[1 + groups][...] = ins[0][...]
        if put is not None:
            outs[1 + groups][...] = ins[2 * n + 1][...]

    ins = [p.spec(BM // n, D, lambda j, i, o: (i, 0)) for p in grad]
    ins += [p.spec(BM // n, BN, lambda j, i, o: (i, j)) for p in hidden]
    ins.append((w_down, pl.BlockSpec((None, BN, D), lambda j, i, o: (layer, o[MINE] if half else j, 0))))

    def out(m):
        return (jax.ShapeDtypeStruct((m, PIECE, cols), BF16), pl.BlockSpec((m, BM // n, BN), lambda j, i, o: (0, i, j)))

    kept = [(jax.ShapeDtypeStruct((PIECE, D), BF16), pl.BlockSpec((BM // n, D), lambda j, i, o: (i, 0)))] if keep else []
    aliases = None
    if put is not None:
        ins += [(put[0], pl.BlockSpec((64, D), lambda j, i, o: (8 * j + i, 0))), (put[1], ANY_SPEC)]
        kept = [(STACK, pl.BlockSpec((None, 64, D), lambda j, i, o: (1, 16 * o[THEIRS] + 8 * j + i, 0)))]
        aliases = {2 * n + 2: 1 + groups}
    *res, tok = call(body, (cols // BN, n * PIECE // BM), ins, [out(n)] + [out(2)] * groups + kept, 2 * n * PIECE * D * cols, order, token, aliases)
    return res[0], res[1:], tok


def hidden_again(order, token, x, w_up, layer, half):
    n = len(x)
    cols = BN if half else F

    def body(ins, outs):
        h = lax.dot_general(join(ins[:n]), ins[n][...], NN, preferred_element_type=jnp.float32)
        outs[0][...] = h.reshape(n, BM // n, BN).astype(BF16)

    ins = [p.spec(BM // n, D, lambda j, i, o: (i, 0)) for p in x]
    ins.append((w_up, pl.BlockSpec((None, D, BN), lambda j, i, o: (layer, 0, o[MINE] if half else j))))
    out = (jax.ShapeDtypeStruct((n, PIECE, cols), BF16), pl.BlockSpec((n, BM // n, BN), lambda j, i, o: (0, i, j)))
    return call(body, (cols // BN, n * PIECE // BM), ins, [out], 2 * n * PIECE * D * cols, order, token)


def back_term(order, token, d_mine, d_core, w_mine, w_core, layer):
    n = 2

    def body(ins, outs):
        left = jnp.concatenate([join(ins[:n]), join(ins[n:2 * n])], axis=1)
        acc = lax.dot_general(left, join(ins[2 * n:2 * n + 2], 1), NT, preferred_element_type=jnp.float32)
        for k in range(n):
            outs[k][...] = acc[k * (BM // n):(k + 1) * (BM // n)].astype(BF16)

    ins = [p.spec(BM // n, F, lambda j, i, o: (i, 0)) for p in parts(d_mine) + parts(d_core)]
    ins += [(w, pl.BlockSpec((None, BN, F), lambda j, i, o: (layer, j, 0))) for w in (w_mine, w_core)]
    outs = [(jax.ShapeDtypeStruct((PIECE, D), BF16), pl.BlockSpec((BM // n, BN), lambda j, i, o: (i, j)))] * n
    return call(body, (D // BN, n * PIECE // BM), ins, outs, 4 * n * PIECE * D * F, order, token)


def weight_grad(order, token, left, right, left_cols, right_cols, bn, ins_more, outs, add, aliases):
    n = len(left)
    (grid_i, at_i), (grid_j, at_j) = left_cols, right_cols

    def body(ins, outs):
        acc = lax.dot_general(join(ins[:n]), join(ins[n:2 * n]), TN, preferred_element_type=jnp.float32)
        if add:
            acc = acc + ins[2 * n][...]
        for o in outs:
            o[...] = acc

    ins = [p.spec(PIECE, BN, lambda i, j, o: (0, at_i(i, o))) for p in left]
    ins += [p.spec(PIECE, bn, lambda i, j, o: (0, at_j(j, o))) for p in right]
    return call(body, (grid_i, grid_j), ins + ins_more, outs, 2 * n * PIECE * grid_i * BN * grid_j * bn, order, token,
                None if aliases is None else {2 * n + k: v for k, v in aliases.items()})


STACK = jax.ShapeDtypeStruct((2, 2048, 2048), jnp.float32)


def weight_full(order, token, left, right, total, add):
    tile = pl.BlockSpec((None, BN, BN), lambda i, j, o: (0, i, j))
    step = (2, lambda k, o: k)
    return weight_grad(order, token, left, right, step, step, BN, [(total, tile if add else ANY_SPEC)], [(STACK, tile)], add, {0: 0})


def weight_last(order, token, left, right, total, pieces):
    n, bn = len(left), 512
    tile = pl.BlockSpec((None, BN, bn), lambda i, j, o: (0, i, j))

    def body(ins, outs):
        acc = lax.dot_general(join(ins[:n]), join(ins[n:2 * n]), TN, preferred_element_type=jnp.float32)
        outs[0][...] = acc + ins[2 * n][...]
        step = 4 * pl.program_id(0) + pl.program_id(1)
        for k in range(3):
            @pl.when(step // 2 == k)
            def _(k=k):
                outs[1][...] = ins[2 * n + 1 + k][...]

    def row(i, j):
        return jnp.minimum(4 * i + j, 5)

    ins = [p.spec(PIECE, BN, lambda i, j, o: (0, i)) for p in left]
    ins += [p.spec(PIECE, bn, lambda i, j, o: (0, j)) for p in right]
    ins.append((total, tile))
    ins += [p.spec(BM, D, lambda i, j, o, k=k: (jnp.clip(4 * i + j - 2 * k, 0, 1), 0)) for k, p in enumerate(pieces)]
    outs = [(STACK, tile),
            (jax.ShapeDtypeStruct((4, PIECE, D), BF16), pl.BlockSpec((None, BM, D), lambda i, j, o: (o[row(i, j) // 2], row(i, j) % 2, 0)))]
    return call(body, (2, 4), ins, outs, 2 * n * PIECE * 2048 * 2048, order, token, {2 * n: 0})


def weight_half(order, token, left, right, down, prev):
    bn = 512
    if down:
        shape = jax.ShapeDtypeStruct((BN, D), jnp.float32)
        cols = ((1, lambda k, o: o[MINE] if prev is None else 0), (4, lambda k, o: k))
        at = lambda i, j, o: (1, o[MINE], j)
    else:
        shape = jax.ShapeDtypeStruct((D, BN), jnp.float32)
        cols = ((2, lambda k, o: k), (2, lambda k, o: 2 * o[MINE] + k if prev is None else k))
        at = lambda i, j, o: (1, i, 2 * o[MINE] + j)
    tile = pl.BlockSpec((BN, bn), lambda i, j, o: (i, j))
    outs = [(shape, tile)]
    if prev is not None:
        outs.append((STACK, pl.BlockSpec((None, BN, bn), at)))
    return weight_grad(order, token, left, right, *cols, bn, [] if prev is None else [(prev, tile)], outs, prev is not None, None)


def finish(order, token, last, grad, up_in, up):
    def body(ins, outs):
        outs[0][...] = ins[0][...]
        outs[1][...] = ins[1][...]

    ins = [last.spec(256, D, lambda i, o: (i, 0)), (up_in, pl.BlockSpec((512, BN), lambda i, o: (i, 0))), (grad, ANY_SPEC), (up, ANY_SPEC)]
    outs = [(jax.ShapeDtypeStruct((4, PIECE, D), BF16), pl.BlockSpec((None, 256, D), lambda i, o: (o[3], i, 0))),
            (STACK, pl.BlockSpec((None, 512, BN), lambda i, o: (1, i, o[THEIRS])))]
    return call(body, (4,), ins, outs, 1000, order, token, {2: 0, 3: 1})


def f32(v):
    return v.astype(jnp.float32)


def solution(mesh):
    def steps(w_up, w_down, x_saved, h_saved, grad_out):
        order, sub = device_order()
        tok = jnp.zeros((8, 128), jnp.float32)
        x_nat = x_saved.reshape(2, 4, PIECE, D)
        h_nat = h_saved.reshape(2, 4, PIECE, F)
        g_nat = grad_out.reshape(4, PIECE, D)

        def my_half(block, which):
            return lax.dynamic_slice(block, (which * BM, 0), (BM, D))

        def both_halves(mine, other):
            return jnp.where(sub == 0, jnp.concatenate([mine, other]), jnp.concatenate([other, mine]))

        def own_block(arr, lead, after):
            idx = (lead, order[0] + after[0, 0].astype(jnp.int32), 0, 0)
            return lax.dynamic_slice(arr, idx, (1, 1, PIECE, D)).reshape(PIECE, D)

        def summed(p02, near, which):
            return f32(my_half(p02, which)) + f32(my_half(near, which))

        x1z = send(own_block(x_nat, 1, tok), PERM_Z)
        w_core = send(w_up, PERM_C)
        g2 = natural(g_nat)
        a1, (dm, do, g2mine), tok = hidden_grad(order, tok, g2, natural(h_nat, 1), w_down, 1, False, True)
        g2z = send(g2mine, PERM_Z)
        dc = send(do, PERM_C)
        down_h, tok = weight_half(order, tok, parts(a1), g2, True, None)
        x1c0 = send(x1z, PERM_C)
        x1s = send(x1z, PERM_S1)
        p02, p13, tok = back_term(order, tok, dm, dc, w_up, w_core, 1)
        near = send(p13, PERM_S1)
        x1c1 = send(x1s, PERM_C)
        hp, tok = hidden_again(order, tok, whole(x1z, x1c0, x1s, x1c1), w_up, 1, True)
        x0z = send(own_block(x_nat, 0, tok), PERM_Z)
        g2c0 = send(g2z, PERM_C)
        g2s = send(g2z, PERM_S1)
        far = send(summed(p02, near, 1 - sub).astype(BF16), PERM_S2)
        apa, (dpa,), tok = hidden_grad(order, tok, whole(g2z, g2c0), [Piece(hp, 0), Piece(hp, 1)], w_down, 1, True)
        up_h, tok = weight_half(order, tok, natural(x_nat, 1), parts(dm) + parts(do), False, None)
        g1m0 = (f32(my_half(g2mine, sub)) + (summed(p02, near, sub) + f32(far))).astype(BF16)
        g1m2 = send(g1m0, PERM_S2)
        g2s, _ = lax.optimization_barrier((g2s, g1m0))
        g2c1 = send(g2s, PERM_C)
        apb, (dpb,), tok = hidden_grad(order, tok, whole(g2s, g2c1), [Piece(hp, 2), Piece(hp, 3)], w_down, 1, True)
        g1mine = both_halves(g1m0, g1m2)
        g1s = send(g1mine, PERM_S1)
        g1c0 = send(g1mine, PERM_C)
        g1zp = send(g1mine, PERM_Z)
        down_h, down, tok = weight_half(order, tok, parts(apa) + parts(apb), whole(g2z, g2c0, g2s, g2c1), True, down_h)
        down_in = send(down_h, PERM_Z)
        up_h, up, tok = weight_half(order, tok, whole(x1z, x1c0, x1s, x1c1), parts(dpa) + parts(dpb), False, up_h)
        g1c1 = send(g1s, PERM_C)
        up_in = send(up_h, PERM_Z)

        g1 = whole(g1mine, g1s, g1c0, g1c1)
        a0, (dm, do), tok = hidden_grad(order, tok, g1, natural(h_nat, 0), w_down, 0, False)
        dc = send(do, PERM_C)
        x0c0 = send(x0z, PERM_C)
        x0s = send(x0z, PERM_S1)
        down, tok = weight_full(order, tok, parts(a0), g1, down, False)
        x0c1 = send(x0s, PERM_C)
        g1cp0 = send(g1zp, PERM_C)
        g1sp = send(g1zp, PERM_S1)
        p02, p13, tok = back_term(order, tok, dm, dc, w_up, w_core, 0)
        near = send(p13, PERM_S1)
        g1cp1 = send(g1sp, PERM_C)
        up, tok = weight_full(order, tok, natural(x_nat, 0), parts(dm) + parts(do), up, False)
        far = send(summed(p02, near, 1 - sub).astype(BF16), PERM_S2)
        hp, tok = hidden_again(order, tok, whole(x0z, x0c0, x0s, x0c1), w_up, 0, False)
        g0m0 = (f32(g1m0) + (summed(p02, near, sub) + f32(far))).astype(BF16)
        g0m2 = send(g0m0, PERM_S2)
        g1p = whole(g1zp, g1cp0, g1sp, g1cp1)
        ap, (dma, dmb, down), tok = hidden_grad(order, tok, g1p, parts(hp), w_down, 0, False, put=(down_in, down))
        g0mine = both_halves(g0m0, g0m2)
        g0s = send(g0mine, PERM_S1)
        g0c0 = send(g0mine, PERM_C)
        up, tok = weight_full(order, tok, whole(x0z, x0c0, x0s, x0c1), parts(dma) + parts(dmb), up, True)
        g0c1 = send(g0s, PERM_C)
        down, grad_in, tok = weight_last(order, tok, parts(ap), g1p, down, whole(g0mine, g0s, g0c0))
        grad_in, up, tok = finish(order, tok, Piece(g0c1), grad_in, up_in, up)
        return grad_in.reshape(1, 4 * PIECE, D), up, down

    body = jax.shard_map(
        steps, mesh=mesh,
        in_specs=(P(None, None, "tp"), P(None, "tp", None), P(None, "dp", None, None), P(None, "dp", None, "tp"), P("dp", None, None)),
        out_specs=(P("dp", None, None), P(None, None, "tp"), P(None, "tp", None)), check_vma=False)
    shapes = ((2, D, 16384), (2, 16384, D), (2, 2, 4096, D), (2, 2, 4096, 16384), (2, 4096, D))
    jax.eval_shape(body, *[jax.ShapeDtypeStruct(s, BF16) for s in shapes])
    return body
```
